32 devices in a mesh: gx: 2 (over y), gy: 4 (over z), gz: 4 (over x, core).
Axes of the slice: x: 2, y: 2, z: 4, core: 2. Of those that a mesh axis runs over, the one named last changes fastest.
Arguments:
- velocity: float32 [8192, 3, 128], P(('gx', 'gy', 'gz')), may hold values from -6 to 6
- cell_index: int32 [8192, 128], P(('gx', 'gy', 'gz')), may hold values from 0 to 5804
- block_target: int32 [8192, 1], P(('gx', 'gy', 'gz')), may hold values from 0 to 31; in each aligned block of 256 rows (0 to 255, 256 to 511, ...) at most 12 rows name the same one
- rotation_axis: int32 [32, 32, 32], replicated, may hold values from 0 to 63
- grid_shift: int32 [3], replicated, may hold values from 0 to 31
Outputs:
- brick_velocity: float32 [32, 32, 12, 3, 128], P(('gx', 'gy', 'gz'))
- cell_flow: float32 [3, 8, 32, 512], P(None, 'gx', 'gy', 'gz')
The draws below stay inside these ranges and needn't reach their ends.
Inputs may be any that keep to these rules, and one draw needn't show every extreme that they name: `block_target`: among the blocks that one device holds, no brick is named by more than 12 blocks, a bound that some block reaches.
All inputs are finite; a program needn't handle non-finite values.
Results may differ from the reference program's by a relative error of at most 0.0003.
Values sent between devices are 32-bit elements; how exact they have to be, the bound alone decides.
A program may use at most 64 MiB of HBM per device.

```python
import math
import jax
import jax.numpy as jnp
import numpy as np
from jax import lax

CX = 4
CY = 8
CZ = 128
BLK_DEV = 256
BROWS = 128
NAX = 64
APER = 32
MOST = 12
NBLK = 8192
NCX = 8
NCY = 32
NCZ = 512
N_GY = 4
N_GZ = 4
DEVICES = 32


def with_ends(entries, rng, least, largest):
    spot = [jax.random.randint(jax.random.fold_in(rng, axis), (), 0, length) for axis, length in enumerate(entries.shape)]
    main_axis = entries.shape.index(max(entries.shape))
    neighbour = spot[:main_axis] + [(spot[main_axis] + 1) % entries.shape[main_axis]] + spot[main_axis + 1:]
    return entries.at[tuple(spot)].set(least).at[tuple(neighbour)].set(largest)


def shard_levels(stream_key, extent, cuts, least, high):
    factor_of = 1.0
    for axis_at, parts in cuts:
        draws = jax.random.uniform(jax.random.fold_in(jax.random.fold_in(stream_key, 6), axis_at), (parts,), jnp.float32, least / len(cuts), high / len(cuts))
        factor_of = factor_of * jnp.repeat(jnp.exp(draws), extent[axis_at] // parts).reshape((-1,) + (1,) * (len(extent) - 1 - axis_at))
    return factor_of


def routed_block(key, own, number, rows, amount, top, limit, slope):
    sequence = jax.random.permutation(key, amount)
    packed, common = load_shares(amount, rows * top, limit, slope, True), load_shares(amount, rows * top, limit, slope, False)
    places = jnp.arange(amount)

    def named(tallies, rotation):
        used = int((tallies > 0).sum())
        fixed = max(1, used // 4)
        moved = fixed + (places - fixed + rotation * (used - fixed)) % max(1, amount - fixed)
        return jnp.zeros((amount,), jnp.int32).at[sequence[jnp.where(places < fixed, places, moved)]].set(jnp.asarray(tallies, jnp.int32))

    tallies = jnp.where(number % 4 == 0, named(packed, number // 4), named(common, number - number // 4 - 1))
    mixed = jax.random.permutation(jax.random.fold_in(own, 3), amount)
    source_of, sink = mixed[0:amount // 2 * 2:2], mixed[1:amount // 2 * 2:2]
    room = jnp.minimum(tallies[source_of] - 1, limit - tallies[sink]) // 2
    room = jnp.where((source_of == sequence[0]) | (sink == sequence[0]) | (tallies[sink] == 0), 0, jnp.maximum(room, 0))
    moved = jax.random.randint(jax.random.fold_in(own, 4), (amount // 2,), 0, 1 << 20) % (room + 1)
    tallies = tallies.at[source_of].add(-moved).at[sink].add(moved)
    members = jnp.searchsorted(jnp.cumsum(tallies), jnp.arange(rows * top), side="right").astype(jnp.int32)
    table = members.reshape(top, rows).T
    table = table[jax.random.permutation(jax.random.fold_in(own, 1), rows)]
    rotation = jax.random.randint(jax.random.fold_in(own, 2), (rows, 1), 0, top)
    return jnp.take_along_axis(table, (jnp.arange(top)[None, :] + rotation) % top, axis=1)


def load_shares(amount, total, most, skew, full):
    portions = [(1 << 20) // math.isqrt(grade ** skew) + 1 for grade in range(1, amount + 1)]
    largest = most if full else min(most, max(-(-total // amount), total * portions[0] // sum(portions)))
    least = 1 if total - largest >= amount - 1 else 0
    given, surplus = [largest] + [least] * (amount - 1), total - largest - least * (amount - 1)
    while surplus > 0:
        movable = [i for i in range(1, amount) if given[i] < largest] or [i for i in range(1, amount) if given[i] < most]
        mass, left = sum([portions[i] for i in movable]), surplus
        for i in movable:
            addition = min(most - given[i], max(1, left * portions[i] // mass), surplus)
            given[i] = given[i] + addition
            surplus = surplus - addition
    return np.array(given)


def normal_values(key, dims, spread, limit, split=(), kind=jnp.bfloat16):
    values = spread * jax.random.normal(key, dims, jnp.float32)
    if split:
        values = values * shard_levels(key, dims, split, -0.22, 0.18)
    return jnp.clip(values, -limit, limit).astype(kind)


def setup_inputs(seed: int = 0) -> dict:
    splits = jax.random.split(jax.random.key(seed), 6)
    velocity = normal_values(splits[0], (NBLK, 3, BROWS), 1.0, 6.0, ((0, 32),), jnp.float32)
    cell_index = with_ends(jax.random.randint(splits[1], (NBLK, BROWS), 0, (CX + 1) * (CY + 1) * (CZ + 1)), jax.random.fold_in(splits[1], 1), 0, ((CX + 1) * (CY + 1) * (CZ + 1)) - 1).astype(jnp.int32)
    block_target_keys = jax.random.split(jax.random.fold_in(splits[2], 1), NBLK // BLK_DEV)
    block_target_turns = jax.random.permutation(jax.random.fold_in(splits[2], 3), NBLK // BLK_DEV)
    block_target = jax.vmap(lambda own, number: routed_block(jax.random.fold_in(splits[2], 2), own, number, BLK_DEV, DEVICES, 1, MOST, 1))(block_target_keys, block_target_turns).reshape((NBLK, 1))
    rotation_axis = with_ends(jax.random.randint(splits[3], (APER, APER, APER), 0, NAX), jax.random.fold_in(splits[3], 1), 0, NAX - 1).astype(jnp.int32)
    grid_shift = jax.random.randint(splits[4], (3,), 0, APER).astype(jnp.int32)
    return dict(velocity=velocity, cell_index=cell_index, block_target=block_target, rotation_axis=rotation_axis, grid_shift=grid_shift)


angle_cosine = -0.6427876096865393
angle_sine = 0.766044443118978

def axis_table():
    counter = jnp.arange(NAX, dtype=jnp.float32) + 0.5
    height = 1.0 - 2.0 * counter / NAX
    radius = jnp.sqrt(jnp.maximum(1.0 - height * height, 0.0))
    turning = counter * 2.399963229728653
    return jnp.stack([radius * jnp.cos(turning), radius * jnp.sin(turning), height])

def rotate_about(direction, relative):
    inner_product = direction[0] * relative[0] + direction[1] * relative[1] + direction[2] * relative[2]
    crossed = [direction[1] * relative[2] - direction[2] * relative[1], direction[2] * relative[0] - direction[0] * relative[2], direction[0] * relative[1] - direction[1] * relative[0]]
    return [relative[component] * angle_cosine + crossed[component] * angle_sine + direction[component] * inner_product * (1.0 - angle_cosine) for component in range(3)]

def reference(velocity, cell_index, block_target, rotation_axis, grid_shift):
    blocks = velocity.shape[0]
    devices = blocks // BLK_DEV
    target = block_target[:, 0]

    def ranks_of(targets):
        onehot = (targets[:, None] == jnp.arange(devices, dtype=jnp.int32)[None, :]).astype(jnp.int32)
        return lax.optimization_barrier(jnp.sum((jnp.cumsum(onehot, axis=0) - onehot) * onehot, axis=1))
    ranking = lax.map(ranks_of, target.reshape(devices, BLK_DEV)).reshape(blocks)
    sender = jnp.arange(blocks, dtype=jnp.int32) // BLK_DEV
    brick_x = target // (N_GY * N_GZ)
    brick_y = target // N_GZ % N_GY
    brick_z = target % N_GZ
    plane_cells = (CY + 1) * (CZ + 1)
    local_x = cell_index // plane_cells
    local_y = cell_index // (CZ + 1) % (CY + 1)
    local_z = cell_index % (CZ + 1)
    global_x = (brick_x[:, None] * CX + local_x) % NCX
    global_y = (brick_y[:, None] * CY + local_y) % NCY
    global_z = (brick_z[:, None] * CZ + local_z) % NCZ
    flat_cell = ((global_x * NCY + global_y) * NCZ + global_z).reshape(-1)
    moving = jnp.transpose(velocity, (1, 0, 2)).reshape(3, -1)
    cell_count = NCX * NCY * NCZ
    counts = jax.ops.segment_sum(jnp.ones(flat_cell.shape, jnp.float32), flat_cell, num_segments=cell_count)
    moments = jnp.stack([jax.ops.segment_sum(moving[component], flat_cell, num_segments=cell_count) for component in range(3)])
    cell_means = moments / jnp.maximum(counts, 1.0)
    cell_flow = cell_means.reshape(3, NCX, NCY, NCZ)
    picked = rotation_axis[(global_x + grid_shift[0]) % APER, (global_y + grid_shift[1]) % APER, (global_z + grid_shift[2]) % APER].reshape(-1)
    direction = axis_table()[:, picked]
    local_flow = cell_means[:, flat_cell]
    relative = [moving[component] - local_flow[component] for component in range(3)]
    turned = rotate_about(direction, relative)
    updated = jnp.stack([local_flow[component] + turned[component] for component in range(3)])
    updated = jnp.transpose(updated.reshape(3, blocks, BROWS), (1, 0, 2))
    places = (target * devices + sender) * MOST + ranking
    placed = jnp.zeros((devices * devices * MOST, 3, BROWS), jnp.float32).at[places].set(updated)
    brick_velocity = placed.reshape(devices, devices, MOST, 3, BROWS)
    return (brick_velocity, cell_flow)
```

```python
import functools
import jax
import jax.numpy as jnp
from jax import lax
from jax.experimental import pallas as pl
from jax.experimental.pallas import tpu as pltpu
from jax.sharding import PartitionSpec as P

CX = 4
CY = 8
CZ = 128
NAX = 64
APER = 32
PLANES = (CX + 1) * (CY + 1)
HALF = 24
ROWS = 2 * HALF
WIDE = 2 * CZ
STEP = 8


angle_cosine = -0.6427876096865393
angle_sine = 0.766044443118978
highest = lax.Precision.HIGHEST


def with_halo(cells, sides, width):
    for axis, dim in sides:
        count = lax.axis_size(axis)
        head = lax.slice_in_dim(cells, 0, width, axis=dim)
        tail = lax.slice_in_dim(cells, cells.shape[dim] - width, cells.shape[dim], axis=dim)
        cells = jnp.concatenate(
            [
                lax.ppermute(tail, axis, [(i, (i + 1) % count) for i in range(count)]),
                cells,
                lax.ppermute(head, axis, [((i + 1) % count, i) for i in range(count)]),
            ],
            axis=dim,
        )
    return cells


def axis_table():
    counter = jnp.arange(NAX, dtype=jnp.float32) + 0.5
    height = 1.0 - 2.0 * counter / NAX
    radius = jnp.sqrt(jnp.maximum(1.0 - height * height, 0.0))
    turning = counter * 2.399963229728653
    return jnp.stack([radius * jnp.cos(turning), radius * jnp.sin(turning), height])


def rotate_about(direction, relative):
    inner_product = (
        direction[0] * relative[0] + direction[1] * relative[1] + direction[2] * relative[2]
    )
    crossed = [
        direction[1] * relative[2] - direction[2] * relative[1],
        direction[2] * relative[0] - direction[0] * relative[2],
        direction[0] * relative[1] - direction[1] * relative[0],
    ]
    return [
        relative[component] * angle_cosine
        + crossed[component] * angle_sine
        + direction[component] * inner_product * (1.0 - angle_cosine)
        for component in range(3)
    ]


def fold_rims(padded, dimension, length):
    inside = lax.slice_in_dim(padded, 1, length + 1, axis=dimension)
    lowest = lax.slice_in_dim(padded, 0, 1, axis=dimension)
    highest_rim = lax.slice_in_dim(padded, length + 1, length + 2, axis=dimension)
    position = lax.broadcasted_iota(jnp.int32, inside.shape, dimension)
    return (
        inside
        + jnp.where(position == 0, lowest, 0.0)
        + jnp.where(position == length - 1, highest_rim, 0.0)
    )


def lookup_table(rotation_axis, index_x, index_y, index_z):
    table = rotation_axis.astype(jnp.float32)
    pick_x = (index_x[:, None] == jnp.arange(APER, dtype=jnp.int32)[None, :]).astype(jnp.float32)
    pick_y = (index_y[:, None] == jnp.arange(APER, dtype=jnp.int32)[None, :]).astype(jnp.float32)
    pick_z = (index_z[:, None] == jnp.arange(APER, dtype=jnp.int32)[None, :]).astype(jnp.float32)
    section = jnp.einsum("xa,abc->xbc", pick_x, table, precision=highest)
    section = jnp.einsum("xbc,yb->xyc", section, pick_y, precision=highest)
    section = jnp.einsum("xyc,zc->xyz", section, pick_z, precision=highest)
    return (section + 0.5).astype(jnp.int32)


def pack_kernel(capacity, target_ref, velocity_ref, cell_ref, out_ref, code_ref, count_ref):
    blocks = velocity_ref.shape[0]
    devices = count_ref.shape[0]
    cell = cell_ref[...]
    plane = (cell * 8129) >> 20
    depth = cell - plane * (CZ + 1)
    inner = depth < CZ
    row = jnp.where(inner, plane, PLANES)
    lane = jnp.where(inner, depth, plane)
    upper = row >= HALF
    code_ref[...] = jnp.where(
        upper, (row - HALF) * WIDE + CZ + lane, row * WIDE + lane
    ).astype(jnp.float32)
    component = lax.broadcasted_iota(jnp.int32, out_ref.shape, 1)
    out_ref[...] = jnp.where(component == 3, -1.0, 0.0)

    def clear(d, carry):
        count_ref[d] = 0
        return carry

    lax.fori_loop(0, devices, clear, 0)

    def place(b, carry):
        target = target_ref[b]
        rank = count_ref[target]
        count_ref[target] = rank + 1
        slot = target * capacity + rank
        out_ref[slot, 0:3, :] = velocity_ref[b]
        out_ref[slot, 3:4, :] = code_ref[pl.ds(b, 1), :]
        return carry

    lax.fori_loop(0, blocks, place, 0, unroll=4)


def code_onehots(labels):
    code = labels.astype(jnp.int32)
    row = code >> 8
    column = code & (WIDE - 1)
    width = labels.shape[1]
    by_row = lax.broadcasted_iota(jnp.int32, (HALF, width), 0) == row
    by_column = lax.broadcasted_iota(jnp.int32, (WIDE, width), 0) == column
    return by_row, by_column.astype(jnp.float32).astype(jnp.bfloat16)


def scatter_kernel(x_ref, out_ref, total_ref, left_ref, right_ref):
    slots = x_ref.shape[0]
    total_ref[...] = jnp.zeros_like(total_ref)

    def step(i, carry):
        for j in range(STEP):
            data = x_ref[i * STEP + j]
            by_row, by_column = code_onehots(data[3:4])
            right_ref[:, j * CZ : (j + 1) * CZ] = by_column
            moving = data[0:3]
            upper = moving.astype(jnp.bfloat16).astype(jnp.float32)
            lower = moving - upper
            parts = [jnp.where(by_row, 1.0, 0.0)]
            for source in (upper, lower):
                for component in range(3):
                    parts.append(jnp.where(by_row, source[component : component + 1], 0.0))
            left_ref[:, j * CZ : (j + 1) * CZ] = jnp.concatenate(parts, axis=0).astype(jnp.bfloat16)
        total_ref[...] += lax.dot_general(
            left_ref[...],
            right_ref[...],
            (((1,), (1,)), ((), ())),
            preferred_element_type=jnp.float32,
        )
        return carry

    lax.fori_loop(0, slots // STEP, step, 0)
    for channel in range(4):
        value = total_ref[channel * HALF : (channel + 1) * HALF, :]
        if channel > 0:
            value = value + total_ref[(channel + 3) * HALF : (channel + 4) * HALF, :]
        out_ref[channel, 0:HALF, :] = value[:, 0:CZ]
        out_ref[channel, HALF:ROWS, :] = value[:, CZ:WIDE]


def gather_kernel(x_ref, table_ref, out_ref, held_ref):
    slots = x_ref.shape[0]
    for channel in range(6):
        value = jnp.concatenate(
            [table_ref[channel, 0:HALF, :], table_ref[channel, HALF:ROWS, :]], axis=1
        )
        upper = value.astype(jnp.bfloat16)
        held_ref[channel * HALF : (channel + 1) * HALF, :] = upper
        held_ref[(channel + 6) * HALF : (channel + 7) * HALF, :] = (
            value - upper.astype(jnp.float32)
        ).astype(jnp.bfloat16)

    def step(i, carry):
        for j in range(0, STEP, 2):
            first = i * STEP + j
            data = jnp.concatenate([x_ref[first], x_ref[first + 1]], axis=1)
            labels = data[3:4]
            by_row, by_column = code_onehots(labels)
            read = jnp.dot(held_ref[...], by_column, preferred_element_type=jnp.float32)
            picked = []
            for channel in range(6):
                value = (
                    read[channel * HALF : (channel + 1) * HALF]
                    + read[(channel + 6) * HALF : (channel + 7) * HALF]
                )
                picked.append(jnp.sum(jnp.where(by_row, value, 0.0), axis=0, keepdims=True))
            relative = [data[c : c + 1] - picked[c] for c in range(3)]
            turned = rotate_about(picked[3:], relative)
            for c in range(3):
                updated = jnp.where(labels >= 0.0, picked[c] + turned[c], 0.0)
                out_ref[first, c : c + 1, :] = updated[:, 0:CZ]
                out_ref[first + 1, c : c + 1, :] = updated[:, CZ:WIDE]
        return carry

    lax.fori_loop(0, slots // STEP, step, 0)


def local_call(kernel, out_shape, in_spaces, scratch, operations):
    return pl.pallas_call(
        kernel,
        out_shape=jax.ShapeDtypeStruct(out_shape, jnp.float32),
        in_specs=[pl.BlockSpec(memory_space=space) for space in in_spaces],
        out_specs=pl.BlockSpec(memory_space=pltpu.VMEM),
        scratch_shapes=scratch,
        cost_estimate=pl.CostEstimate(
            flops=operations, bytes_accessed=1 << 20, transcendentals=0
        ),
    )


def to_rows(cells):
    main = cells[..., :CZ].reshape(-1, PLANES, CZ)
    rim = cells[..., CZ].reshape(-1, 1, PLANES)
    rim = jnp.pad(rim, ((0, 0), (0, ROWS - PLANES - 1), (0, CZ - PLANES)))
    return jnp.concatenate([main, rim], axis=1)


def shards(velocity, cell_index, block_target, rotation_axis, grid_shift):
    devices = lax.axis_size(("gx", "gy", "gz"))
    blocks = velocity.shape[0]
    block_rows = velocity.shape[2]
    capacity = 3 * blocks // (2 * devices)
    slots = devices * capacity
    packed = local_call(
        functools.partial(pack_kernel, capacity),
        (slots, 4, block_rows),
        (pltpu.SMEM, pltpu.VMEM, pltpu.VMEM),
        [pltpu.VMEM((blocks, block_rows), jnp.float32), pltpu.SMEM((devices,), jnp.int32)],
        1 << 20,
    )(block_target[:, 0], velocity, cell_index)
    arriving = lax.all_to_all(
        packed.reshape(devices, capacity, 4, block_rows),
        ("gx", "gy", "gz"),
        split_axis=0,
        concat_axis=0,
        tiled=True,
    ).reshape(slots, 4, block_rows)
    totals = local_call(
        scatter_kernel,
        (4, ROWS, CZ),
        (pltpu.VMEM,),
        [
            pltpu.VMEM((7 * HALF, WIDE), jnp.float32),
            pltpu.VMEM((7 * HALF, STEP * CZ), jnp.bfloat16),
            pltpu.VMEM((WIDE, STEP * CZ), jnp.bfloat16),
        ],
        1 << 33,
    )(arriving)
    main = totals[:, :PLANES].reshape(4, CX + 1, CY + 1, CZ)
    rim = totals[:, PLANES, :PLANES].reshape(4, CX + 1, CY + 1, 1)
    partial_value = jnp.concatenate([main, rim], axis=3)
    folded = fold_rims(with_halo(partial_value, (("gx", 1),), 1), 1, CX + 1)
    folded = fold_rims(with_halo(folded, (("gy", 2),), 1), 2, CY + 1)
    folded = fold_rims(with_halo(folded, (("gz", 3),), 1), 3, CZ + 1)
    cell_means = folded[1:] / jnp.maximum(folded[0], 1.0)
    cell_flow = cell_means[:, :CX, :CY, :CZ]
    index_x = (
        (lax.axis_index("gx") * CX + jnp.arange(CX + 1, dtype=jnp.int32))
        % (CX * lax.axis_size("gx"))
        + grid_shift[0]
    ) % APER
    index_y = (
        (lax.axis_index("gy") * CY + jnp.arange(CY + 1, dtype=jnp.int32))
        % (CY * lax.axis_size("gy"))
        + grid_shift[1]
    ) % APER
    index_z = (
        (lax.axis_index("gz") * CZ + jnp.arange(CZ + 1, dtype=jnp.int32))
        % (CZ * lax.axis_size("gz"))
        + grid_shift[2]
    ) % APER
    picked = lookup_table(rotation_axis, index_x, index_y, index_z).reshape(-1)
    choose = (jnp.arange(NAX, dtype=jnp.int32)[:, None] == picked[None, :]).astype(jnp.float32)
    direction = jnp.dot(axis_table(), choose, precision=highest)
    table = jnp.concatenate(
        [cell_means, direction.reshape(3, CX + 1, CY + 1, CZ + 1)], axis=0
    )
    updated = local_call(
        gather_kernel,
        (slots, 3, block_rows),
        (pltpu.VMEM, pltpu.VMEM),
        [pltpu.VMEM((12 * HALF, WIDE), jnp.bfloat16)],
        1 << 33,
    )(arriving, to_rows(table))
    return (updated.reshape(1, devices, capacity, 3, block_rows), cell_flow)


def solution(mesh):
    return jax.shard_map(
        shards,
        mesh=mesh,
        in_specs=(
            P(("gx", "gy", "gz"), None, None),
            P(("gx", "gy", "gz"), None),
            P(("gx", "gy", "gz"), None),
            P(),
            P(),
        ),
        out_specs=(P(("gx", "gy", "gz"), None, None, None, None), P(None, "gx", "gy", "gz")),
        check_vma=False,
    )
```

```python
import functools
import jax
import jax.numpy as jnp
from jax import lax
from jax.experimental import pallas as pl
from jax.experimental.pallas import tpu as pltpu
from jax.sharding import PartitionSpec as P

CX = 4
CY = 8
CZ = 128
NAX = 64
APER = 32
PLANES = (CX + 1) * (CY + 1)
HALF = 24
ROWS = 2 * HALF
WIDE = 2 * CZ
STEP = 8


angle_cosine = -0.6427876096865393
angle_sine = 0.766044443118978
highest = lax.Precision.HIGHEST


def with_halo(cells, sides, width):
    for axis, dim in sides:
        count = lax.axis_size(axis)
        head = lax.slice_in_dim(cells, 0, width, axis=dim)
        tail = lax.slice_in_dim(cells, cells.shape[dim] - width, cells.shape[dim], axis=dim)
        cells = jnp.concatenate(
            [
                lax.ppermute(tail, axis, [(i, (i + 1) % count) for i in range(count)]),
                cells,
                lax.ppermute(head, axis, [((i + 1) % count, i) for i in range(count)]),
            ],
            axis=dim,
        )
    return cells


def axis_table():
    counter = jnp.arange(NAX, dtype=jnp.float32) + 0.5
    height = 1.0 - 2.0 * counter / NAX
    radius = jnp.sqrt(jnp.maximum(1.0 - height * height, 0.0))
    turning = counter * 2.399963229728653
    return jnp.stack([radius * jnp.cos(turning), radius * jnp.sin(turning), height])


def rotate_about(direction, relative):
    inner_product = (
        direction[0] * relative[0] + direction[1] * relative[1] + direction[2] * relative[2]
    )
    crossed = [
        direction[1] * relative[2] - direction[2] * relative[1],
        direction[2] * relative[0] - direction[0] * relative[2],
        direction[0] * relative[1] - direction[1] * relative[0],
    ]
    return [
        relative[component] * angle_cosine
        + crossed[component] * angle_sine
        + direction[component] * inner_product * (1.0 - angle_cosine)
        for component in range(3)
    ]


def fold_rims(padded, dimension, length):
    inside = lax.slice_in_dim(padded, 1, length + 1, axis=dimension)
    lowest = lax.slice_in_dim(padded, 0, 1, axis=dimension)
    highest_rim = lax.slice_in_dim(padded, length + 1, length + 2, axis=dimension)
    position = lax.broadcasted_iota(jnp.int32, inside.shape, dimension)
    return (
        inside
        + jnp.where(position == 0, lowest, 0.0)
        + jnp.where(position == length - 1, highest_rim, 0.0)
    )


def lookup_table(rotation_axis, index_x, index_y, index_z):
    table = rotation_axis.astype(jnp.float32)
    pick_x = (index_x[:, None] == jnp.arange(APER, dtype=jnp.int32)[None, :]).astype(jnp.float32)
    pick_y = (index_y[:, None] == jnp.arange(APER, dtype=jnp.int32)[None, :]).astype(jnp.float32)
    pick_z = (index_z[:, None] == jnp.arange(APER, dtype=jnp.int32)[None, :]).astype(jnp.float32)
    section = jnp.einsum("xa,abc->xbc", pick_x, table, precision=highest)
    section = jnp.einsum("xbc,yb->xyc", section, pick_y, precision=highest)
    section = jnp.einsum("xyc,zc->xyz", section, pick_z, precision=highest)
    return (section + 0.5).astype(jnp.int32)


def pack_kernel(sizes, target_ref, velocity_ref, cell_ref, first_ref, second_ref, code_ref, count_ref):
    blocks = velocity_ref.shape[1]
    devices = count_ref.shape[0]
    cell = cell_ref[...]
    plane = (cell * 8129) >> 20
    depth = cell - plane * (CZ + 1)
    inner = depth < CZ
    row = jnp.where(inner, plane, PLANES)
    lane = jnp.where(inner, depth, plane)
    upper = row >= HALF
    code_ref[...] = jnp.where(
        upper, (row - HALF) * WIDE + CZ + lane, row * WIDE + lane
    ).astype(jnp.float32)
    for out_ref in (first_ref, second_ref):
        component = lax.broadcasted_iota(jnp.int32, out_ref.shape, 1)
        out_ref[...] = jnp.where(component == 3, -1.0, 0.0)

    def clear(d, carry):
        count_ref[d] = 0
        return carry

    lax.fori_loop(0, devices, clear, 0)

    def place(b, carry):
        target = target_ref[b]
        rank = count_ref[target]
        count_ref[target] = rank + 1

        def put(out_ref, slot):
            for component in range(3):
                out_ref[slot, component : component + 1, :] = velocity_ref[component, pl.ds(b, 1), :]
            out_ref[slot, 3:4, :] = code_ref[pl.ds(b, 1), :]

        @pl.when(rank < sizes[0])
        def early():
            put(first_ref, target * sizes[0] + rank)

        @pl.when(rank >= sizes[0])
        def late():
            put(second_ref, target * sizes[1] + rank - sizes[0])

        return carry

    lax.fori_loop(0, blocks, place, 0, unroll=4)


def code_onehots(labels):
    code = labels.astype(jnp.int32)
    row = code >> 8
    column = code & (WIDE - 1)
    width = labels.shape[1]
    by_row = lax.broadcasted_iota(jnp.int32, (HALF, width), 0) == row
    by_column = lax.broadcasted_iota(jnp.int32, (WIDE, width), 0) == column
    return by_row, by_column.astype(jnp.float32).astype(jnp.bfloat16)


def scatter_kernel(x_ref, before_ref, out_ref, total_ref, left_ref, right_ref):
    slots = x_ref.shape[0]
    for channel in range(4):
        total_ref[channel * HALF : (channel + 1) * HALF, 0:CZ] = before_ref[channel, 0:HALF, :]
        total_ref[channel * HALF : (channel + 1) * HALF, CZ:WIDE] = before_ref[channel, HALF:ROWS, :]
    total_ref[4 * HALF : 7 * HALF, :] = jnp.zeros((3 * HALF, WIDE), jnp.float32)

    def step(i, carry):
        for j in range(STEP):
            data = x_ref[i * STEP + j]
            by_row, by_column = code_onehots(data[3:4])
            right_ref[:, j * CZ : (j + 1) * CZ] = by_column
            moving = data[0:3]
            upper = moving.astype(jnp.bfloat16).astype(jnp.float32)
            lower = moving - upper
            parts = [jnp.where(by_row, 1.0, 0.0)]
            for source in (upper, lower):
                for component in range(3):
                    parts.append(jnp.where(by_row, source[component : component + 1], 0.0))
            left_ref[:, j * CZ : (j + 1) * CZ] = jnp.concatenate(parts, axis=0).astype(jnp.bfloat16)
        total_ref[...] += lax.dot_general(
            left_ref[...],
            right_ref[...],
            (((1,), (1,)), ((), ())),
            preferred_element_type=jnp.float32,
        )
        return carry

    lax.fori_loop(0, slots // STEP, step, 0)
    for channel in range(4):
        value = total_ref[channel * HALF : (channel + 1) * HALF, :]
        if channel > 0:
            value = value + total_ref[(channel + 3) * HALF : (channel + 4) * HALF, :]
        out_ref[channel, 0:HALF, :] = value[:, 0:CZ]
        out_ref[channel, HALF:ROWS, :] = value[:, CZ:WIDE]


def gather_kernel(sizes, first_ref, second_ref, table_ref, out_ref, held_ref):
    devices = out_ref.shape[2]
    groups = devices // STEP
    for channel in range(6):
        value = jnp.concatenate(
            [table_ref[channel, 0:HALF, :], table_ref[channel, HALF:ROWS, :]], axis=1
        )
        upper = value.astype(jnp.bfloat16)
        held_ref[channel * HALF : (channel + 1) * HALF, :] = upper
        held_ref[(channel + 6) * HALF : (channel + 7) * HALF, :] = (
            value - upper.astype(jnp.float32)
        ).astype(jnp.bfloat16)

    def read_from(x_ref, size, offset):
        def step(i, carry):
            rank = i // groups
            sender = (i % groups) * STEP
            blocks = [x_ref[(sender + j) * size + rank] for j in range(STEP)]
            picked = [[] for channel in range(6)]
            for j in range(0, STEP, 2):
                labels = jnp.concatenate([blocks[j][3:4], blocks[j + 1][3:4]], axis=1)
                by_row, by_column = code_onehots(labels)
                read = jnp.dot(held_ref[...], by_column, preferred_element_type=jnp.float32)
                for channel in range(6):
                    value = (
                        read[channel * HALF : (channel + 1) * HALF]
                        + read[(channel + 6) * HALF : (channel + 7) * HALF]
                    )
                    row = jnp.sum(jnp.where(by_row, value, 0.0), axis=0, keepdims=True)
                    picked[channel] += [row[:, 0:CZ], row[:, CZ:WIDE]]
            held = [jnp.concatenate(rows, axis=0) for rows in picked]
            own = [
                jnp.concatenate([block[c : c + 1] for block in blocks], axis=0) for c in range(4)
            ]
            relative = [own[c] - held[c] for c in range(3)]
            turned = rotate_about(held[3:], relative)
            place = pl.ds(pl.multiple_of(sender, STEP), STEP)
            for c in range(3):
                out_ref[offset + rank, c, place, :] = jnp.where(
                    own[3] >= 0.0, held[c] + turned[c], 0.0
                )
            return carry

        lax.fori_loop(0, size * groups, step, 0)

    read_from(first_ref, sizes[0], 0)
    read_from(second_ref, sizes[1], sizes[0])


def local_call(kernel, out_shape, in_spaces, scratch, operations):
    return pl.pallas_call(
        kernel,
        out_shape=[jax.ShapeDtypeStruct(shape, jnp.float32) for shape in out_shape],
        in_specs=[pl.BlockSpec(memory_space=space) for space in in_spaces],
        out_specs=[pl.BlockSpec(memory_space=pltpu.VMEM) for shape in out_shape],
        scratch_shapes=scratch,
        cost_estimate=pl.CostEstimate(
            flops=operations, bytes_accessed=1 << 20, transcendentals=0
        ),
    )


def to_rows(cells):
    main = cells[..., :CZ].reshape(-1, PLANES, CZ)
    rim = cells[..., CZ].reshape(-1, 1, PLANES)
    rim = jnp.pad(rim, ((0, 0), (0, ROWS - PLANES - 1), (0, CZ - PLANES)))
    return jnp.concatenate([main, rim], axis=1)


def shards(velocity, cell_index, block_target, rotation_axis, grid_shift):
    devices = lax.axis_size(("gx", "gy", "gz"))
    blocks = velocity.shape[0]
    block_rows = velocity.shape[2]
    capacity = 3 * blocks // (2 * devices)
    sizes = (capacity // 2, capacity - capacity // 2)
    packed = local_call(
        functools.partial(pack_kernel, sizes),
        [(devices * size, 4, block_rows) for size in sizes],
        (pltpu.SMEM, pltpu.VMEM, pltpu.VMEM),
        [pltpu.VMEM((blocks, block_rows), jnp.float32), pltpu.SMEM((devices,), jnp.int32)],
        1 << 20,
    )(block_target[:, 0], jnp.transpose(velocity, (1, 0, 2)), cell_index)
    arrived = []
    totals = jnp.zeros((4, ROWS, CZ), jnp.float32)
    for size, outgoing in zip(sizes, packed):
        arrived.append(
            lax.all_to_all(
                outgoing.reshape(devices, size, 4, block_rows),
                ("gx", "gy", "gz"),
                split_axis=0,
                concat_axis=0,
                tiled=True,
            ).reshape(devices * size, 4, block_rows)
        )
    for arriving in arrived:
        totals = local_call(
            scatter_kernel,
            [(4, ROWS, CZ)],
            (pltpu.VMEM, pltpu.VMEM),
            [
                pltpu.VMEM((7 * HALF, WIDE), jnp.float32),
                pltpu.VMEM((7 * HALF, STEP * CZ), jnp.bfloat16),
                pltpu.VMEM((WIDE, STEP * CZ), jnp.bfloat16),
            ],
            1 << 33,
        )(arriving, totals)[0]
    main = totals[:, :PLANES].reshape(4, CX + 1, CY + 1, CZ)
    rim = totals[:, PLANES, :PLANES].reshape(4, CX + 1, CY + 1, 1)
    partial_value = jnp.concatenate([main, rim], axis=3)
    folded = fold_rims(with_halo(partial_value, (("gx", 1),), 1), 1, CX + 1)
    folded = fold_rims(with_halo(folded, (("gy", 2),), 1), 2, CY + 1)
    folded = fold_rims(with_halo(folded, (("gz", 3),), 1), 3, CZ + 1)
    cell_means = folded[1:] / jnp.maximum(folded[0], 1.0)
    cell_flow = cell_means[:, :CX, :CY, :CZ]
    index_x = (
        (lax.axis_index("gx") * CX + jnp.arange(CX + 1, dtype=jnp.int32))
        % (CX * lax.axis_size("gx"))
        + grid_shift[0]
    ) % APER
    index_y = (
        (lax.axis_index("gy") * CY + jnp.arange(CY + 1, dtype=jnp.int32))
        % (CY * lax.axis_size("gy"))
        + grid_shift[1]
    ) % APER
    index_z = (
        (lax.axis_index("gz") * CZ + jnp.arange(CZ + 1, dtype=jnp.int32))
        % (CZ * lax.axis_size("gz"))
        + grid_shift[2]
    ) % APER
    picked = lookup_table(rotation_axis, index_x, index_y, index_z).reshape(-1)
    choose = (jnp.arange(NAX, dtype=jnp.int32)[:, None] == picked[None, :]).astype(jnp.float32)
    direction = jnp.dot(axis_table(), choose, precision=highest)
    table = jnp.concatenate(
        [cell_means, direction.reshape(3, CX + 1, CY + 1, CZ + 1)], axis=0
    )
    updated = local_call(
        functools.partial(gather_kernel, sizes),
        [(capacity, 3, devices, block_rows)],
        (pltpu.VMEM, pltpu.VMEM, pltpu.VMEM),
        [pltpu.VMEM((12 * HALF, WIDE), jnp.bfloat16)],
        1 << 33,
    )(*arrived, to_rows(table))[0]
    return (jnp.transpose(updated, (2, 0, 1, 3))[None], cell_flow)


def solution(mesh):
    return jax.shard_map(
        shards,
        mesh=mesh,
        in_specs=(
            P(("gx", "gy", "gz"), None, None),
            P(("gx", "gy", "gz"), None),
            P(("gx", "gy", "gz"), None),
            P(),
            P(),
        ),
        out_specs=(P(("gx", "gy", "gz"), None, None, None, None), P(None, "gx", "gy", "gz")),
        check_vma=False,
    )
```
